8 devices in a mesh: tp: 4 (over z, y, x), ep: 2 (over core).
Axes of the slice: x: 2, y: 2, z: 1, core: 2. Of those that a mesh axis runs over, the one named last changes fastest.
Arguments:
- hidden_in: bfloat16 [1024, 2048], P(('tp', 'ep'))
- kv_cache0: bfloat16 [1024, 64, 576], P(('tp', 'ep'))
- kv_cache1: bfloat16 [1024, 64, 576], P(('tp', 'ep'))
- kv_lens: int32 [1024], P(('tp', 'ep'))
- route_ids: int32 [1024, 6], P(('tp', 'ep'))
- route_wts: float32 [1024, 6], P(('tp', 'ep'))
- attn0_q: bfloat16 [2048, 16, 192], replicated
- attn0_uk: bfloat16 [16, 128, 512], replicated
- attn0_uv: bfloat16 [16, 512, 128], replicated
- attn0_out: bfloat16 [16, 128, 2048], replicated
- attn1_q: bfloat16 [2048, 16, 192], replicated
- attn1_uk: bfloat16 [16, 128, 512], replicated
- attn1_uv: bfloat16 [16, 512, 128], replicated
- attn1_out: bfloat16 [16, 128, 2048], replicated
- ffn0_gate: bfloat16 [2048, 10944], P(None, 'tp')
- ffn0_up: bfloat16 [2048, 10944], P(None, 'tp')
- ffn0_down: bfloat16 [10944, 2048], P('tp')
- ffn1_gate: bfloat16 [2048, 10944], P(None, 'tp')
- ffn1_up: bfloat16 [2048, 10944], P(None, 'tp')
- ffn1_down: bfloat16 [10944, 2048], P('tp')
- exp_gate: bfloat16 [64, 2048, 1408], P(('tp', 'ep'))
- exp_up: bfloat16 [64, 2048, 1408], P(('tp', 'ep'))
- exp_down: bfloat16 [64, 1408, 2048], P(('tp', 'ep'))
Outputs:
- output: bfloat16 [1024, 2048], P(('tp', 'ep'))
All inputs are finite; a program needn't handle non-finite values.
Results may differ from the reference program's by a relative error of at most 0.0167883.
Values are sent between devices in bfloat16 or wider.
A program may use at most 1.25 GiB of HBM per device.

```python
import jax
import jax.numpy as jnp
from jax import lax

HIDDEN = 2048
EXPERTS = 64
ZERO = 0
TOPK = 6
EXP_FF = 1408
HEADS = 16
NOPE = 128
ROPE = 64
LATENT = 512
VDIM = 128
DENSE_FF = 10944
BATCH = 128
CTX = 64
DEVICES = 8
MAX_CHIPS = 4

CHIPS = DEVICES // 2
TOKENS = DEVICES * BATCH
EXP_LOCAL = EXPERTS // DEVICES
CAP = (BATCH * MAX_CHIPS + CHIPS - 1) // CHIPS
EXPERT_CAP = min(TOKENS, DEVICES * CAP)


def draw_routing(route_key):
    key_chip, key_tok, key_off, key_zero, key_zid, key_len = jax.random.split(route_key, 6)
    chip_perm = jax.vmap(lambda sub_key: jax.random.permutation(sub_key, CHIPS))(jax.random.split(key_chip, DEVICES))
    tok_perm = jax.vmap(lambda sub_key: jax.random.permutation(sub_key, BATCH))(jax.random.split(key_tok, DEVICES))
    slot_pos = jnp.arange(TOPK)
    chip_slot = slot_pos % MAX_CHIPS
    rank_slot = slot_pos // MAX_CHIPS
    chip_pos = (tok_perm[:, :, None] * MAX_CHIPS + chip_slot[None, None, :]) % CHIPS
    chip_of = jnp.take_along_axis(chip_perm, chip_pos.reshape(DEVICES, BATCH * TOPK), axis=1).reshape(DEVICES, BATCH, TOPK)
    chip_off = jax.random.randint(key_off, (DEVICES, BATCH, MAX_CHIPS), 0, 2 * EXP_LOCAL)
    local_id = (chip_off[:, :, chip_slot] + rank_slot) % (2 * EXP_LOCAL)
    routed = chip_of * (2 * EXP_LOCAL) + local_id
    zero_pick = (jax.random.randint(key_zero, (DEVICES, BATCH, TOPK), 0, 4) == 0) & (slot_pos >= MAX_CHIPS) & (ZERO > 0)
    zero_base = jax.random.randint(key_zid, (DEVICES, BATCH, 1), 0, max(ZERO, 1))
    zero_id = EXPERTS + (zero_base + slot_pos) % max(ZERO, 1)
    route_ids = jnp.where(zero_pick, zero_id, routed).reshape(TOKENS, TOPK).astype(jnp.int32)
    kv_lens = jax.random.randint(key_len, (TOKENS,), 1, CTX + 1).at[0].set(CTX).astype(jnp.int32)
    return route_ids, kv_lens


def setup_inputs(seed: int = 0) -> dict:
    keys = jax.random.split(jax.random.key(seed), 24)
    route_ids, kv_lens = draw_routing(keys[0])

    def normal_w(sub_key, shape, fan_in, gain):
        return (jax.random.normal(sub_key, shape, jnp.float32) * (gain * fan_in ** -0.5)).astype(jnp.bfloat16)

    return {
        'hidden_in': jax.random.normal(keys[1], (TOKENS, HIDDEN), jnp.float32).astype(jnp.bfloat16),
        'kv_cache0': jax.random.normal(keys[2], (TOKENS, CTX, LATENT + ROPE), jnp.float32).astype(jnp.bfloat16),
        'kv_cache1': jax.random.normal(keys[3], (TOKENS, CTX, LATENT + ROPE), jnp.float32).astype(jnp.bfloat16),
        'kv_lens': kv_lens,
        'route_ids': route_ids,
        'route_wts': jax.random.uniform(keys[4], (TOKENS, TOPK), jnp.float32, 0.5, 1.5),
        'attn0_q': normal_w(keys[5], (HIDDEN, HEADS, NOPE + ROPE), HIDDEN, 1.0),
        'attn0_uk': normal_w(keys[6], (HEADS, NOPE, LATENT), NOPE, 1.0),
        'attn0_uv': normal_w(keys[7], (HEADS, LATENT, VDIM), LATENT, 1.0),
        'attn0_out': normal_w(keys[8], (HEADS, VDIM, HIDDEN), HEADS * VDIM, 4.0),
        'attn1_q': normal_w(keys[9], (HIDDEN, HEADS, NOPE + ROPE), HIDDEN, 1.0),
        'attn1_uk': normal_w(keys[10], (HEADS, NOPE, LATENT), NOPE, 1.0),
        'attn1_uv': normal_w(keys[11], (HEADS, LATENT, VDIM), LATENT, 1.0),
        'attn1_out': normal_w(keys[12], (HEADS, VDIM, HIDDEN), HEADS * VDIM, 4.0),
        'ffn0_gate': normal_w(keys[13], (HIDDEN, DENSE_FF), HIDDEN, 1.0),
        'ffn0_up': normal_w(keys[14], (HIDDEN, DENSE_FF), HIDDEN, 1.0),
        'ffn0_down': normal_w(keys[15], (DENSE_FF, HIDDEN), DENSE_FF, 1.0),
        'ffn1_gate': normal_w(keys[16], (HIDDEN, DENSE_FF), HIDDEN, 1.0),
        'ffn1_up': normal_w(keys[17], (HIDDEN, DENSE_FF), HIDDEN, 1.0),
        'ffn1_down': normal_w(keys[18], (DENSE_FF, HIDDEN), DENSE_FF, 1.0),
        'exp_gate': normal_w(keys[19], (EXPERTS, HIDDEN, EXP_FF), HIDDEN, 1.0),
        'exp_up': normal_w(keys[20], (EXPERTS, HIDDEN, EXP_FF), HIDDEN, 1.0),
        'exp_down': normal_w(keys[21], (EXPERTS, EXP_FF, HIDDEN), EXP_FF, 1.0),
    }


def rms_norm(values):
    vals_f = values.astype(jnp.float32)
    return (vals_f * lax.rsqrt(jnp.mean(vals_f * vals_f, axis=-1, keepdims=True) + 1e-6)).astype(jnp.bfloat16)


def rope_rotate(q_rope, kv_lens):
    half_dim = ROPE // 2
    inv_freq = 10000.0 ** (-2.0 * jnp.arange(half_dim, dtype=jnp.float32) / ROPE)
    rot_angle = kv_lens.astype(jnp.float32)[:, None, None] * inv_freq
    cos_a = jnp.cos(rot_angle)
    sin_a = jnp.sin(rot_angle)
    q_first = q_rope[..., :half_dim].astype(jnp.float32)
    q_second = q_rope[..., half_dim:].astype(jnp.float32)
    return jnp.concatenate([q_first * cos_a - q_second * sin_a, q_second * cos_a + q_first * sin_a], axis=-1).astype(jnp.bfloat16)


def mla_block(hidden, kv_cache, kv_lens, w_q, w_uk, w_uv, w_out):
    normed = rms_norm(hidden)
    q_all = jnp.einsum('bh,hnd->bnd', normed.astype(jnp.float32), w_q.astype(jnp.float32)).astype(jnp.bfloat16)
    q_lat = jnp.einsum('bnd,ndl->bnl', q_all[..., :NOPE].astype(jnp.float32), w_uk.astype(jnp.float32)).astype(jnp.bfloat16)
    q_full = jnp.concatenate([q_lat, rope_rotate(q_all[..., NOPE:], kv_lens)], axis=-1)
    cache_f = kv_cache.astype(jnp.float32)
    scores = jnp.einsum('bnc,bkc->bnk', q_full.astype(jnp.float32), cache_f) * (NOPE + ROPE) ** -0.5
    pos_mask = jnp.arange(CTX)[None, None, :] < kv_lens[:, None, None]
    attn_probs = jax.nn.softmax(jnp.where(pos_mask, scores, -1e30), axis=-1).astype(jnp.bfloat16)
    o_lat = jnp.einsum('bnk,bkl->bnl', attn_probs.astype(jnp.float32), cache_f[..., :LATENT]).astype(jnp.bfloat16)
    o_head = jnp.einsum('bnl,nlv->bnv', o_lat.astype(jnp.float32), w_uv.astype(jnp.float32)).astype(jnp.bfloat16)
    return jnp.einsum('bnv,nvh->bh', o_head.astype(jnp.float32), w_out.astype(jnp.float32))


def attend(hidden, kv_cache, kv_lens, w_q, w_uk, w_uv, w_out):
    blocks = (hidden.reshape(DEVICES, BATCH, HIDDEN), kv_cache.reshape(DEVICES, BATCH, CTX, LATENT + ROPE), kv_lens.reshape(DEVICES, BATCH))
    out_blocks = lax.map(lambda block_args: mla_block(block_args[0], block_args[1], block_args[2], w_q, w_uk, w_uv, w_out), blocks)
    return out_blocks.reshape(TOKENS, HIDDEN)


def swiglu(normed, w_gate, w_up, w_down):
    gate_out = jnp.dot(normed, w_gate, preferred_element_type=jnp.float32)
    up_out = jnp.dot(normed, w_up, preferred_element_type=jnp.float32)
    act_val = (jax.nn.silu(gate_out) * up_out).astype(jnp.bfloat16)
    return jnp.dot(act_val, w_down, preferred_element_type=jnp.float32)


def routed_experts(normed, route_ids, route_wts, exp_gate, exp_up, exp_down):
    padded = jnp.concatenate([normed, jnp.zeros((1, HIDDEN), normed.dtype)], axis=0)

    def one_expert(moe_acc, expert_idx):
        tok_hit = route_ids == expert_idx
        hit_wts = jnp.concatenate([jnp.sum(jnp.where(tok_hit, route_wts, 0.0), axis=1), jnp.zeros((1,), jnp.float32)])
        tok_idx = jnp.nonzero(jnp.any(tok_hit, axis=1), size=EXPERT_CAP, fill_value=TOKENS)[0]
        down_out = swiglu(padded[tok_idx], exp_gate[expert_idx], exp_up[expert_idx], exp_down[expert_idx])
        return moe_acc.at[tok_idx].add(down_out * hit_wts[tok_idx][:, None]), None

    moe_acc, scan_out = lax.scan(one_expert, jnp.zeros((TOKENS + 1, HIDDEN), jnp.float32), jnp.arange(EXPERTS))
    zero_wts = jnp.sum(jnp.where(route_ids >= EXPERTS, route_wts, 0.0), axis=1)
    return moe_acc[:TOKENS] + zero_wts[:, None] * normed.astype(jnp.float32)


def reference(hidden_in, kv_cache0, kv_cache1, kv_lens, route_ids, route_wts, attn0_q, attn0_uk, attn0_uv, attn0_out, attn1_q, attn1_uk, attn1_uv, attn1_out, ffn0_gate, ffn0_up, ffn0_down, ffn1_gate, ffn1_up, ffn1_down, exp_gate, exp_up, exp_down):
    attn_zero = attend(hidden_in, kv_cache0, kv_lens, attn0_q, attn0_uk, attn0_uv, attn0_out)
    state_h0 = (hidden_in.astype(jnp.float32) + attn_zero).astype(jnp.bfloat16)
    normed0 = rms_norm(state_h0)
    moe_out = routed_experts(normed0, route_ids, route_wts, exp_gate, exp_up, exp_down)
    state_f0 = (state_h0.astype(jnp.float32) + swiglu(normed0, ffn0_gate, ffn0_up, ffn0_down)).astype(jnp.bfloat16)
    attn_one = attend(state_f0, kv_cache1, kv_lens, attn1_q, attn1_uk, attn1_uv, attn1_out)
    state_h1 = (state_f0.astype(jnp.float32) + attn_one).astype(jnp.bfloat16)
    ffn_one = swiglu(rms_norm(state_h1), ffn1_gate, ffn1_up, ffn1_down)
    return (state_h1.astype(jnp.float32) + ffn_one + moe_out).astype(jnp.bfloat16)
```

```python
import functools

import jax
import jax.numpy as jnp
from jax import lax
from jax.experimental import pallas as pl
from jax.experimental.pallas import tpu as pltpu
from jax.sharding import PartitionSpec as P

EPS = 1e-6
ROPE_BASE = 10000.0
BF = jnp.bfloat16
F32 = jnp.float32
NT = (((1,), (1,)), ((), ()))
TN = (((0,), (0,)), ((), ()))
VMEM_BYTES = 67043328


def dot_nn(lhs, rhs):
    return jnp.dot(lhs, rhs, preferred_element_type=F32)


def dot_nt(lhs, rhs):
    return lax.dot_general(lhs, rhs, NT, preferred_element_type=F32)


def dot_tn(lhs, rhs):
    return lax.dot_general(lhs, rhs, TN, preferred_element_type=F32)


def rms_f32(vals_f):
    return (vals_f * lax.rsqrt(jnp.mean(vals_f * vals_f, axis=-1, keepdims=True) + EPS)).astype(BF)


KV_STEP = 8
TOK_GROUP = 16


def mla_kernel(n_extra, heads, nope, rope, lat, vdim, ctx, *refs):
    x_ref = refs[0]
    extra = refs[1:1 + n_extra]
    (lens_ref, cos_ref, sin_ref, kv_hbm, wq_hbm, uk_hbm, uv_hbm, wo_hbm,
     h_ref, u_ref,
     kv_in, wqn, wqr, uk, uv, wo, kv_s, q_s, o_s, oh_s, xs, sem_kv, sem_w) = refs[1 + n_extra:]
    batch, hidden = x_ref.shape
    n_grp = batch // TOK_GROUP
    n_kv = ctx // KV_STEP

    def kv_copy(step):
        return pltpu.make_async_copy(kv_hbm.at[pl.ds(step * KV_STEP, KV_STEP)], kv_in.at[pl.ds(step * KV_STEP, KV_STEP)], sem_kv.at[step])

    cps = []
    for head in range(heads):
        cps.append(pltpu.make_async_copy(wq_hbm.at[head, pl.ds(0, nope), :], wqn.at[pl.ds(head * nope, nope), :], sem_w.at[0]))
        cps.append(pltpu.make_async_copy(wq_hbm.at[head, pl.ds(nope, rope), :], wqr.at[pl.ds(head * rope, rope), :], sem_w.at[1]))
    cp_uk = pltpu.make_async_copy(uk_hbm, uk, sem_w.at[2])
    cp_uv = pltpu.make_async_copy(uv_hbm, uv, sem_w.at[3])
    cp_wo = pltpu.make_async_copy(wo_hbm, wo, sem_w.at[4])
    for step in range(n_kv):
        kv_copy(step).start()
    for cp in cps:
        cp.start()
    cp_uk.start()
    cp_uv.start()
    cp_wo.start()

    hid_f = x_ref[...].astype(F32)
    if n_extra:
        tot = extra[0][...].astype(F32)
        for ref in extra[1:]:
            tot = tot + ref[...].astype(F32)
        hid_f = (hid_f + tot).astype(BF).astype(F32)
    h_ref[...] = hid_f.astype(BF)
    xs[...] = rms_f32(hid_f)

    @pl.loop(0, n_kv)
    def _(step):
        kv_copy(step).wait()
        for sub in range(KV_STEP):
            k_idx = step * KV_STEP + sub
            slab = kv_in[k_idx]
            slab_t = slab.T
            kv_s[:, pl.ds(pl.multiple_of(k_idx * TOK_GROUP, TOK_GROUP), TOK_GROUP), :] = slab_t.reshape(n_grp, TOK_GROUP, lat + rope)

    for cp in cps:
        cp.wait()
    cp_uk.wait()
    x_bf = xs[...]
    hp = 4

    @pl.loop(0, heads // hp)
    def _(blk):
        row0 = pl.multiple_of(blk * hp * nope, hp * nope)
        qn = dot_nt(x_bf, wqn[pl.ds(row0, hp * nope), :]).astype(BF)
        row1 = pl.multiple_of(blk * hp * rope, hp * rope)
        qr = dot_nt(x_bf, wqr[pl.ds(row1, hp * rope), :]).astype(BF)
        for sub in range(hp):
            head = blk * hp + sub
            q_s[head, :, 0:lat] = dot_nn(qn[:, sub * nope:(sub + 1) * nope], uk[head]).astype(BF)
        half = rope // 2
        lane = lax.broadcasted_iota(jnp.int32, (batch, 128), 1) % rope
        for pair in range(hp * rope // 128):
            seg = qr[:, pair * 128:(pair + 1) * 128].astype(F32)
            part = jnp.where(lane < half, pltpu.roll(seg, 128 - half, 1), pltpu.roll(seg, half, 1))
            rot = (seg * cos_ref[...] + part * sin_ref[...])
            per = 128 // rope
            for idx in range(per):
                head = blk * hp + pair * per + idx
                val = rot if idx == 0 else pltpu.roll(rot, 128 - idx * rope, 1)
                q_s[head, :, lat:lat + rope] = val[:, 0:rope].astype(BF)

    scale = (nope + rope) ** -0.5
    rows = heads * TOK_GROUP
    cols = ctx * TOK_GROUP

    @pl.loop(0, n_grp)
    def _(grp):
        tok0 = pl.multiple_of(grp * TOK_GROUP, TOK_GROUP)
        q_g = q_s[:, pl.ds(tok0, TOK_GROUP), :].reshape(rows, lat + rope)
        sc = dot_nt(q_g, kv_s[grp]) * scale
        len_g = lens_ref[pl.ds(tok0, TOK_GROUP), :]
        len_r = jnp.broadcast_to(len_g[None, :, 0:1], (heads, TOK_GROUP, 1)).reshape(rows, 1)
        row_i = lax.broadcasted_iota(jnp.int32, (rows, cols), 0)
        col_i = lax.broadcasted_iota(jnp.int32, (rows, cols), 1)
        ok = ((row_i & (TOK_GROUP - 1)) == (col_i & (TOK_GROUP - 1))) & (lax.shift_right_logical(col_i, 4) < len_r)
        sc = jnp.where(ok, sc, -1e30)
        top = jnp.max(sc, axis=1, keepdims=True)
        pr = jnp.exp(sc - top)
        pr = (pr * (1.0 / jnp.sum(pr, axis=1, keepdims=True))).astype(BF)
        o_g = dot_nn(pr, kv_s[grp, :, 0:lat]).astype(BF)
        o_s[:, pl.ds(tok0, TOK_GROUP), :] = o_g.reshape(heads, TOK_GROUP, lat)

    cp_uv.wait()

    @pl.loop(0, heads // 2)
    def _(blk):
        for sub in range(2):
            head = blk * 2 + sub
            oh_s[:, pl.ds(pl.multiple_of(head * vdim, vdim), vdim)] = dot_nn(o_s[head], uv[head]).astype(BF)

    cp_wo.wait()
    n_step = 512
    oh = oh_s[...]
    ssq = jnp.zeros((batch, 1), F32)
    for col in range(0, hidden, n_step):
        res = h_ref[:, col:col + n_step].astype(F32) + dot_nn(oh, wo[:, col:col + n_step])
        res_b = res.astype(BF)
        h_ref[:, col:col + n_step] = res_b
        res_f = res_b.astype(F32)
        ssq = ssq + jnp.sum(res_f * res_f, axis=1, keepdims=True)
    inv = lax.rsqrt(ssq * (1.0 / hidden) + EPS)
    u_ref[...] = (h_ref[...].astype(F32) * inv).astype(BF)


def mla_call(x, extra, lens_b, cos_t, sin_t, kv_t, wq_t, w_uk, w_uv, w_out):
    batch, hidden = x.shape
    ctx, feat, _ = kv_t.shape
    heads, nope, lat = w_uk.shape
    rope = feat - lat
    vdim = w_uv.shape[2]
    vm = pl.BlockSpec(memory_space=pltpu.VMEM)
    hb = pl.BlockSpec(memory_space=pl.ANY)
    nbytes = 2 * (kv_t.size + wq_t.size + w_uk.size + w_uv.size + w_out.size)
    return pl.pallas_call(
        functools.partial(mla_kernel, len(extra), heads, nope, rope, lat, vdim, ctx),
        out_shape=[jax.ShapeDtypeStruct((batch, hidden), BF)] * 2,
        in_specs=[vm] * (4 + len(extra)) + [hb] * 5,
        out_specs=[vm, vm],
        scratch_shapes=[
            pltpu.VMEM((ctx, feat, batch), BF),
            pltpu.VMEM((heads * nope, hidden), BF),
            pltpu.VMEM((heads * rope, hidden), BF),
            pltpu.VMEM((heads, nope, lat), BF),
            pltpu.VMEM((heads, lat, vdim), BF),
            pltpu.VMEM((heads * vdim, hidden), BF),
            pltpu.VMEM((batch // TOK_GROUP, ctx * TOK_GROUP, feat), BF),
            pltpu.VMEM((heads, batch, feat), BF),
            pltpu.VMEM((heads, batch, lat), BF),
            pltpu.VMEM((batch, heads * vdim), BF),
            pltpu.VMEM((batch, hidden), BF),
            pltpu.SemaphoreType.DMA((ctx // KV_STEP,)),
            pltpu.SemaphoreType.DMA((5,)),
        ],
        compiler_params=pltpu.CompilerParams(vmem_limit_bytes=VMEM_BYTES),
        cost_estimate=pl.CostEstimate(flops=8 * 10 ** 9, bytes_accessed=nbytes, transcendentals=10 ** 6),
        name="mla",
    )(x, *extra, lens_b, cos_t, sin_t, kv_t, wq_t, w_uk, w_uv, w_out.reshape(heads * vdim, hidden))


def ffn_kernel(n_blk, n_add, f_step, *refs):
    x_refs = refs[:n_blk]
    adds = refs[n_blk:n_blk + n_add]
    gate_hbm, up_hbm, down_hbm = refs[n_blk + n_add:n_blk + n_add + 3]
    outs = refs[n_blk + n_add + 3:2 * n_blk + n_add + 3]
    gate, up, down, xs, act, sem = refs[2 * n_blk + n_add + 3:]
    batch = x_refs[0].shape[0]
    ff, hidden = gate.shape
    starts = list(range(0, ff, f_step))
    sizes = [min(f_step, ff - s) for s in starts]

    def cps(idx):
        rows = pl.ds(starts[idx], sizes[idx])
        return [pltpu.make_async_copy(src.at[rows, :], dst.at[rows, :], sem.at[which, idx]) for which, (src, dst) in enumerate(((gate_hbm, gate), (up_hbm, up), (down_hbm, down)))]

    all_cps = [cps(idx) for idx in range(len(starts))]
    for cp in all_cps:
        cp[0].start()
        cp[1].start()
    for cp in all_cps:
        cp[2].start()
    for blk in range(n_blk):
        xs[blk * batch:(blk + 1) * batch, :] = x_refs[blk][...]
    for idx, start in enumerate(starts):
        all_cps[idx][0].wait()
        all_cps[idx][1].wait()
        x_val = xs[...]
        g_val = dot_nt(x_val, gate[start:start + sizes[idx], :])
        u_val = dot_nt(x_val, up[start:start + sizes[idx], :])
        act[:, start:start + sizes[idx]] = (g_val * (1.0 / (1.0 + jnp.exp(-g_val))) * u_val).astype(BF)
    for cp in all_cps:
        cp[2].wait()
    n_step = 512
    for col in range(0, hidden, n_step):
        res = dot_nn(act[...], down[:, col:col + n_step])
        for blk in range(n_blk):
            val = res[blk * batch:(blk + 1) * batch, :]
            for add in adds:
                val = val + add[blk * batch:(blk + 1) * batch, col:col + n_step].astype(F32)
            outs[blk][:, col:col + n_step] = val.astype(BF)


def ffn_call(x_blocks, adds, gate_t, up_t, down):
    n_blk = len(x_blocks)
    batch, hidden = x_blocks[0].shape
    ff = down.shape[0]
    f_step = 512
    n_f = -(-ff // f_step)
    vm = pl.BlockSpec(memory_space=pltpu.VMEM)
    hb = pl.BlockSpec(memory_space=pl.ANY)
    return pl.pallas_call(
        functools.partial(ffn_kernel, n_blk, len(adds), f_step),
        out_shape=[jax.ShapeDtypeStruct((batch, hidden), BF)] * n_blk,
        in_specs=[vm] * (n_blk + len(adds)) + [hb] * 3,
        out_specs=[vm] * n_blk,
        scratch_shapes=[
            pltpu.VMEM((ff, hidden), BF),
            pltpu.VMEM((ff, hidden), BF),
            pltpu.VMEM((ff, hidden), BF),
            pltpu.VMEM((n_blk * batch, hidden), BF),
            pltpu.VMEM((n_blk * batch, ff), BF),
            pltpu.SemaphoreType.DMA((3, n_f)),
        ],
        compiler_params=pltpu.CompilerParams(vmem_limit_bytes=VMEM_BYTES),
        cost_estimate=pl.CostEstimate(flops=6 * n_blk * batch * hidden * ff, bytes_accessed=6 * hidden * ff, transcendentals=n_blk * batch * ff),
        name="ffn",
    )(*x_blocks, *adds, gate_t, up_t, down)


ROW_TILE = 128


def moe_kernel(n_blk, exp_local, ids_ref, wts_ref, base_ref, *refs):
    x_refs = refs[:n_blk]
    gate_ref, up_ref, down_ref, own_ref, sib_ref, xs, acc, rank_s, wrow_s, cnt_s = refs[n_blk:]
    exp = pl.program_id(0)
    top_k, n_tok = ids_ref.shape
    batch, hidden = x_refs[0].shape
    ff = gate_ref.shape[2]

    @pl.when(exp == 0)
    def _():
        for blk in range(n_blk):
            xs[blk * batch:(blk + 1) * batch, :] = x_refs[blk][...]
        acc[...] = jnp.zeros_like(acc)
        local = ids_ref[...] - base_ref[0]
        lane = lax.broadcasted_iota(jnp.int32, (1, n_tok), 1)
        for idx in range(exp_local):
            eq = local == idx
            hit = jnp.max(jnp.where(eq, 1.0, 0.0), axis=0, keepdims=True)
            wrow_s[idx] = jnp.sum(jnp.where(eq, wts_ref[...], 0.0), axis=0, keepdims=True)
            run = hit
            shift = 1
            while shift < n_tok:
                run = run + jnp.where(lane >= shift, pltpu.roll(run, shift, 1), 0.0)
                shift *= 2
            rank_s[idx] = jnp.where(hit > 0.5, run - 1.0, -1.0).astype(jnp.int32)
            cnt_s[idx] = jnp.sum(hit).astype(jnp.int32)

    count = cnt_s[exp]
    rank = rank_s[exp]
    wrow = wrow_s[exp]

    def tile(step, carry):
        row_i = lax.broadcasted_iota(jnp.int32, (ROW_TILE, n_tok), 0) + step * ROW_TILE
        pick = row_i == rank
        pick_b = jnp.where(pick, 1.0, 0.0).astype(BF)
        w_col = jnp.sum(jnp.where(pick, wrow, 0.0), axis=1, keepdims=True)
        x_t = dot_nn(pick_b, xs[...]).astype(BF)
        g_val = dot_nn(x_t, gate_ref[0])
        u_val = dot_nn(x_t, up_ref[0])
        act = (g_val * (1.0 / (1.0 + jnp.exp(-g_val))) * u_val).astype(BF)
        n_step = 512
        for col in range(0, hidden, n_step):
            y_val = (dot_nn(act, down_ref[0, :, col:col + n_step]) * w_col).astype(BF)
            acc[:, col:col + n_step] += dot_tn(pick_b, y_val)
        return carry

    lax.fori_loop(0, (count + ROW_TILE - 1) // ROW_TILE, tile, 0)

    @pl.when(exp == exp_local - 1)
    def _():
        half = n_tok // 2
        own_ref[...] = acc[0:half, :].astype(BF)
        sib_ref[...] = acc[half:n_tok, :].astype(BF)


def moe_call(ids, wts, base, x_blocks, exp_gate, exp_up, exp_down):
    exp_local, hidden, ff = exp_gate.shape
    n_tok = ids.shape[1]
    n_blk = len(x_blocks)
    one = pl.Buffered(1)

    def whole(shape):
        return pl.BlockSpec(shape, lambda e: (0,) * len(shape), pipeline_mode=one)

    return pl.pallas_call(
        functools.partial(moe_kernel, n_blk, exp_local),
        out_shape=[jax.ShapeDtypeStruct((n_tok // 2, hidden), BF)] * 2,
        grid=(exp_local,),
        in_specs=[whole(ids.shape), whole(wts.shape), pl.BlockSpec(memory_space=pltpu.SMEM)]
        + [whole(b.shape) for b in x_blocks]
        + [pl.BlockSpec((1, hidden, ff), lambda e: (e, 0, 0)), pl.BlockSpec((1, hidden, ff), lambda e: (e, 0, 0)), pl.BlockSpec((1, ff, hidden), lambda e: (e, 0, 0))],
        out_specs=[whole((n_tok // 2, hidden))] * 2,
        scratch_shapes=[
            pltpu.VMEM((n_tok, hidden), BF),
            pltpu.VMEM((n_tok, hidden), F32),
            pltpu.VMEM((exp_local, 1, n_tok), jnp.int32),
            pltpu.VMEM((exp_local, 1, n_tok), F32),
            pltpu.SMEM((exp_local,), jnp.int32),
        ],
        compiler_params=pltpu.CompilerParams(dimension_semantics=("arbitrary",), vmem_limit_bytes=VMEM_BYTES),
        cost_estimate=pl.CostEstimate(flops=2 * 10 ** 10, bytes_accessed=6 * exp_gate.size, transcendentals=10 ** 6),
        name="moe",
    )(ids, wts, base, *x_blocks, exp_gate, exp_up, exp_down)


def solution(mesh):
    n_tp = mesh.shape['tp']
    tok_spec = P(('tp', 'ep'))
    rep_spec = P()
    col_spec = P(None, 'tp')
    row_spec = P('tp', None)
    in_specs = (tok_spec, tok_spec, tok_spec, tok_spec, tok_spec, tok_spec, rep_spec, rep_spec, rep_spec, rep_spec, rep_spec, rep_spec, rep_spec, rep_spec, col_spec, col_spec, row_spec, col_spec, col_spec, row_spec, tok_spec, tok_spec, tok_spec)

    def swap_tp(val, bits):
        return lax.ppermute(val, 'tp', [(i, i ^ bits) for i in range(n_tp)])

    def swap_ep(val):
        return lax.ppermute(val, 'ep', [(0, 1), (1, 0)])

    def gather_tp(val):
        return [val] + [swap_tp(val, bits) for bits in range(1, n_tp)]

    def layer_step(hidden_in, kv_cache0, kv_cache1, kv_lens, route_ids, route_wts, attn0_q, attn0_uk, attn0_uv, attn0_out, attn1_q, attn1_uk, attn1_uv, attn1_out, ffn0_gate, ffn0_up, ffn0_down, ffn1_gate, ffn1_up, ffn1_down, exp_gate, exp_up, exp_down):
        batch = hidden_in.shape[0]
        exp_local = exp_gate.shape[0]
        rope = kv_cache0.shape[2] - attn0_uk.shape[2]
        i_tp = lax.axis_index('tp')
        i_ep = lax.axis_index('ep')
        half = rope // 2
        inv_freq = ROPE_BASE ** (-2.0 * jnp.arange(half, dtype=F32) / rope)
        angle = kv_lens.astype(F32)[:, None] * jnp.tile(inv_freq, 128 // half)
        cos_t = jnp.cos(angle)
        sign = jnp.where(jnp.arange(128) % rope < half, -1.0, 1.0).astype(F32)
        sin_t = jnp.sin(angle) * sign
        lens_b = jnp.broadcast_to(kv_lens[:, None], (batch, 128))

        meta = jnp.concatenate([route_ids.T.astype(F32), route_wts.T], axis=0)
        meta_all = lax.all_gather(meta, ('tp', 'ep'), axis=0)
        top_k = route_ids.shape[1]
        order = jnp.stack([(i_tp ^ bits) * 2 + (i_ep ^ sib) for sib in range(2) for bits in range(n_tp)])
        meta_ord = jnp.take(meta_all, order, axis=0)
        meta_ord = jnp.transpose(meta_ord, (1, 0, 2)).reshape(2 * top_k, 2 * n_tp * batch)
        ids_all = meta_ord[:top_k].astype(jnp.int32)
        wts_all = meta_ord[top_k:]
        base = ((i_tp * 2 + i_ep) * exp_local).astype(jnp.int32).reshape(1)

        def t_kv(cache):
            return jnp.transpose(cache, (1, 2, 0))

        h0, u0 = mla_call(hidden_in, [], lens_b, cos_t, sin_t, t_kv(kv_cache0), jnp.transpose(attn0_q, (1, 2, 0)), attn0_uk, attn0_uv, attn0_out)
        u_own = gather_tp(u0)
        u_sib = [swap_ep(b) for b in u_own]
        parts0 = ffn_call(u_own, [], ffn0_gate.T, ffn0_up.T, ffn0_down)
        recv0 = [parts0[0]] + [swap_tp(parts0[bits], bits) for bits in range(1, n_tp)]
        m_own, m_sib = moe_call(ids_all, wts_all, base, u_own + u_sib, exp_gate, exp_up, exp_down)
        m_got = swap_ep(m_sib)
        h1, v0 = mla_call(h0, recv0, lens_b, cos_t, sin_t, t_kv(kv_cache1), jnp.transpose(attn1_q, (1, 2, 0)), attn1_uk, attn1_uv, attn1_out)
        v_own = gather_tp(v0)
        parts1 = ffn_call(v_own, [m_own, m_got], ffn1_gate.T, ffn1_up.T, ffn1_down)
        recv1 = [parts1[0]] + [swap_tp(parts1[bits], bits) for bits in range(1, n_tp)]
        tot = recv1[0].astype(F32) + recv1[1].astype(F32) + recv1[2].astype(F32) + recv1[3].astype(F32)
        return (h1.astype(F32) + tot).astype(BF)

    return jax.shard_map(layer_step, mesh=mesh, in_specs=in_specs, out_specs=tok_spec, check_vma=False)
```

```python
import functools

import jax
import jax.numpy as jnp
from jax import lax
from jax.experimental import pallas as pl
from jax.experimental.pallas import tpu as pltpu
from jax.sharding import PartitionSpec as P

EPS = 1e-6
ROPE_BASE = 10000.0
BF = jnp.bfloat16
F32 = jnp.float32
NT = (((1,), (1,)), ((), ()))
TN = (((0,), (0,)), ((), ()))
VMEM_BYTES = 67043328


def dot_nn(lhs, rhs):
    return jnp.dot(lhs, rhs, preferred_element_type=F32)


def dot_nt(lhs, rhs):
    return lax.dot_general(lhs, rhs, NT, preferred_element_type=F32)


def dot_tn(lhs, rhs):
    return lax.dot_general(lhs, rhs, TN, preferred_element_type=F32)


def rms_f32(vals_f):
    return (vals_f * lax.rsqrt(jnp.mean(vals_f * vals_f, axis=-1, keepdims=True) + EPS)).astype(BF)


KV_STEP = 8
TOK_GROUP = 16


def mla_kernel(n_extra, heads, nope, rope, lat, vdim, ctx, *refs):
    x_ref = refs[0]
    extra = refs[1:1 + n_extra]
    (lens_ref, cos_ref, sin_ref, kv_hbm, wq_hbm, uk_hbm, uv_hbm, wo_hbm,
     h_ref, u_ref,
     kv_in, wqn, wqr, uk, uv, wo, kv_s, q_s, o_s, oh_s, xs, sem_kv, sem_w) = refs[1 + n_extra:]
    batch, hidden = x_ref.shape
    n_grp = batch // TOK_GROUP
    n_kv = ctx // KV_STEP

    def kv_copy(step):
        return pltpu.make_async_copy(kv_hbm.at[pl.ds(step * KV_STEP, KV_STEP)], kv_in.at[pl.ds(step * KV_STEP, KV_STEP)], sem_kv.at[step])

    cps = []
    for head in range(heads):
        cps.append(pltpu.make_async_copy(wq_hbm.at[head, pl.ds(0, nope), :], wqn.at[pl.ds(head * nope, nope), :], sem_w.at[0]))
        cps.append(pltpu.make_async_copy(wq_hbm.at[head, pl.ds(nope, rope), :], wqr.at[pl.ds(head * rope, rope), :], sem_w.at[1]))
    cp_uk = pltpu.make_async_copy(uk_hbm, uk, sem_w.at[2])
    cp_uv = pltpu.make_async_copy(uv_hbm, uv, sem_w.at[3])
    cp_wo = pltpu.make_async_copy(wo_hbm, wo, sem_w.at[4])
    for step in range(n_kv):
        kv_copy(step).start()
    for cp in cps:
        cp.start()
    cp_uk.start()
    cp_uv.start()
    cp_wo.start()

    hid_f = x_ref[...].astype(F32)
    if n_extra:
        tot = extra[0][...].astype(F32)
        for ref in extra[1:]:
            tot = tot + ref[...].astype(F32)
        hid_f = (hid_f + tot).astype(BF).astype(F32)
    h_ref[...] = hid_f.astype(BF)
    xs[...] = rms_f32(hid_f)

    @pl.loop(0, n_kv)
    def _(step):
        kv_copy(step).wait()
        for sub in range(KV_STEP):
            k_idx = step * KV_STEP + sub
            slab = kv_in[k_idx]
            slab_t = slab.T
            kv_s[:, pl.ds(pl.multiple_of(k_idx * TOK_GROUP, TOK_GROUP), TOK_GROUP), :] = slab_t.reshape(n_grp, TOK_GROUP, lat + rope)

    for cp in cps:
        cp.wait()
    cp_uk.wait()
    x_bf = xs[...]
    hp = 4

    @pl.loop(0, heads // hp)
    def _(blk):
        row0 = pl.multiple_of(blk * hp * nope, hp * nope)
        qn = dot_nt(x_bf, wqn[pl.ds(row0, hp * nope), :]).astype(BF)
        row1 = pl.multiple_of(blk * hp * rope, hp * rope)
        qr = dot_nt(x_bf, wqr[pl.ds(row1, hp * rope), :]).astype(BF)
        for sub in range(hp):
            head = blk * hp + sub
            q_s[head, :, 0:lat] = dot_nn(qn[:, sub * nope:(sub + 1) * nope], uk[head]).astype(BF)
        half = rope // 2
        lane = lax.broadcasted_iota(jnp.int32, (batch, 128), 1) % rope
        for pair in range(hp * rope // 128):
            seg = qr[:, pair * 128:(pair + 1) * 128].astype(F32)
            part = jnp.where(lane < half, pltpu.roll(seg, 128 - half, 1), pltpu.roll(seg, half, 1))
            rot = (seg * cos_ref[...] + part * sin_ref[...])
            per = 128 // rope
            for idx in range(per):
                head = blk * hp + pair * per + idx
                val = rot if idx == 0 else pltpu.roll(rot, 128 - idx * rope, 1)
                q_s[head, :, lat:lat + rope] = val[:, 0:rope].astype(BF)

    scale = (nope + rope) ** -0.5
    rows = heads * TOK_GROUP
    cols = ctx * TOK_GROUP

    @pl.loop(0, n_grp)
    def _(grp):
        tok0 = pl.multiple_of(grp * TOK_GROUP, TOK_GROUP)
        q_g = q_s[:, pl.ds(tok0, TOK_GROUP), :].reshape(rows, lat + rope)
        sc = dot_nt(q_g, kv_s[grp]) * scale
        len_g = lens_ref[pl.ds(tok0, TOK_GROUP), :]
        len_r = jnp.broadcast_to(len_g[None, :, 0:1], (heads, TOK_GROUP, 1)).reshape(rows, 1)
        row_i = lax.broadcasted_iota(jnp.int32, (rows, cols), 0)
        col_i = lax.broadcasted_iota(jnp.int32, (rows, cols), 1)
        ok = ((row_i & (TOK_GROUP - 1)) == (col_i & (TOK_GROUP - 1))) & (lax.shift_right_logical(col_i, 4) < len_r)
        sc = jnp.where(ok, sc, -1e30)
        top = jnp.max(sc, axis=1, keepdims=True)
        pr = jnp.exp(sc - top)
        pr = (pr * (1.0 / jnp.sum(pr, axis=1, keepdims=True))).astype(BF)
        o_g = dot_nn(pr, kv_s[grp, :, 0:lat]).astype(BF)
        o_s[:, pl.ds(tok0, TOK_GROUP), :] = o_g.reshape(heads, TOK_GROUP, lat)

    cp_uv.wait()

    @pl.loop(0, heads // 2)
    def _(blk):
        for sub in range(2):
            head = blk * 2 + sub
            oh_s[:, pl.ds(pl.multiple_of(head * vdim, vdim), vdim)] = dot_nn(o_s[head], uv[head]).astype(BF)

    cp_wo.wait()
    n_step = 512
    oh = oh_s[...]
    ssq = jnp.zeros((batch, 1), F32)
    for col in range(0, hidden, n_step):
        res = h_ref[:, col:col + n_step].astype(F32) + dot_nn(oh, wo[:, col:col + n_step])
        res_b = res.astype(BF)
        h_ref[:, col:col + n_step] = res_b
        res_f = res_b.astype(F32)
        ssq = ssq + jnp.sum(res_f * res_f, axis=1, keepdims=True)
    inv = lax.rsqrt(ssq * (1.0 / hidden) + EPS)
    u_ref[...] = (h_ref[...].astype(F32) * inv).astype(BF)


def mla_call(x, extra, lens_b, cos_t, sin_t, kv_t, wq_t, w_uk, w_uv, w_out):
    batch, hidden = x.shape
    ctx, feat, _ = kv_t.shape
    heads, nope, lat = w_uk.shape
    rope = feat - lat
    vdim = w_uv.shape[2]
    vm = pl.BlockSpec(memory_space=pltpu.VMEM)
    hb = pl.BlockSpec(memory_space=pl.ANY)
    nbytes = 2 * (kv_t.size + wq_t.size + w_uk.size + w_uv.size + w_out.size)
    return pl.pallas_call(
        functools.partial(mla_kernel, len(extra), heads, nope, rope, lat, vdim, ctx),
        out_shape=[jax.ShapeDtypeStruct((batch, hidden), BF)] * 2,
        in_specs=[vm] * (4 + len(extra)) + [hb] * 5,
        out_specs=[vm, vm],
        scratch_shapes=[
            pltpu.VMEM((ctx, feat, batch), BF),
            pltpu.VMEM((heads * nope, hidden), BF),
            pltpu.VMEM((heads * rope, hidden), BF),
            pltpu.VMEM((heads, nope, lat), BF),
            pltpu.VMEM((heads, lat, vdim), BF),
            pltpu.VMEM((heads * vdim, hidden), BF),
            pltpu.VMEM((batch // TOK_GROUP, ctx * TOK_GROUP, feat), BF),
            pltpu.VMEM((heads, batch, feat), BF),
            pltpu.VMEM((heads, batch, lat), BF),
            pltpu.VMEM((batch, heads * vdim), BF),
            pltpu.VMEM((batch, hidden), BF),
            pltpu.SemaphoreType.DMA((ctx // KV_STEP,)),
            pltpu.SemaphoreType.DMA((5,)),
        ],
        compiler_params=pltpu.CompilerParams(vmem_limit_bytes=VMEM_BYTES),
        cost_estimate=pl.CostEstimate(flops=8 * 10 ** 9, bytes_accessed=nbytes, transcendentals=10 ** 6),
        name="mla",
    )(x, *extra, lens_b, cos_t, sin_t, kv_t, wq_t, w_uk, w_uv, w_out.reshape(heads * vdim, hidden))


F_STEP = 512
N_STEP = 512
MESH = pl.DeviceIdType.MESH


def silu_mul(g_val, u_val):
    return (g_val * (1.0 / (1.0 + jnp.exp(-g_val))) * u_val).astype(BF)


def weight_copies(pairs, sems, ff):
    starts = list(range(0, ff, F_STEP))
    out = []
    for which, (src, dst) in enumerate(pairs):
        row = []
        for idx, start in enumerate(starts):
            rows = pl.ds(start, min(F_STEP, ff - start))
            row.append(pltpu.make_async_copy(src.at[rows, :], dst.at[rows, :], sems.at[which, idx]))
        out.append(row)
    return out


def ffn_up(copies, first, xs, act, gate, up, tok, n_tok):
    ff = gate.shape[0]
    for idx, start in enumerate(range(0, ff, F_STEP)):
        size = min(F_STEP, ff - start)
        if first:
            copies[0][idx].wait()
            copies[1][idx].wait()
        x_val = xs[tok:tok + n_tok, :]
        g_val = dot_nt(gate[start:start + size, :], x_val)
        u_val = dot_nt(up[start:start + size, :], x_val)
        act[tok:tok + n_tok, start:start + size] = silu_mul(g_val, u_val).T


def peer_barrier(peers):
    barrier = pltpu.get_barrier_semaphore()
    for peer in peers:
        pl.semaphore_signal(barrier, inc=1, device_id=peer, device_id_type=MESH)
    pl.semaphore_wait(barrier, len(peers))


def ffn0_kernel(u_ref, meta_ref, gate_hbm, up_hbm, down_hbm, *refs):
    p0, p1, p2, p3, ua_hbm, ma_ref, gate, up, down, xs, sib, act, msib, sem_w, sem_s, sem_r, sem_m, sem_o = refs
    parts = (p0, p1, p2, p3)
    n_tp = len(parts)
    batch, hidden = u_ref.shape
    ff = gate.shape[0]
    i_tp = lax.axis_index('tp')
    i_ep = lax.axis_index('ep')
    copies = weight_copies(((gate_hbm, gate), (up_hbm, up), (down_hbm, down)), sem_w, ff)
    for idx in range(len(copies[0])):
        copies[0][idx].start()
        copies[1][idx].start()
    for cp in copies[2]:
        cp.start()

    def peer(bits, flip):
        return (jnp.bitwise_xor(i_tp, bits), i_ep + flip - 2 * flip * i_ep)

    peer_barrier([peer(bits, flip) for bits in range(n_tp) for flip in range(2) if bits or flip])

    sends = []
    for bits in range(1, n_tp):
        sends.append(pltpu.make_async_remote_copy(src_ref=u_ref, dst_ref=xs.at[pl.ds(bits * batch, batch), :], send_sem=sem_s.at[bits], recv_sem=sem_r.at[bits], device_id=peer(bits, 0), device_id_type=MESH))
    sib_own = pltpu.make_async_remote_copy(src_ref=u_ref, dst_ref=sib.at[pl.ds(0, batch), :], send_sem=sem_s.at[0], recv_sem=sem_r.at[0], device_id=peer(0, 1), device_id_type=MESH)
    metas = []
    for flip in range(2):
        for bits in range(n_tp):
            if bits or flip:
                slot = flip * n_tp + bits
                metas.append(pltpu.make_async_remote_copy(src_ref=meta_ref, dst_ref=msib.at[slot], send_sem=sem_m.at[0, slot], recv_sem=sem_m.at[1, slot], device_id=peer(bits, flip), device_id_type=MESH))
    sib_own.start()
    for cp in metas:
        cp.start()
    for cp in sends:
        cp.start()
    xs[0:batch, :] = u_ref[...]
    ma_ref[0] = meta_ref[...]
    outs = [pltpu.make_async_copy(u_ref, ua_hbm.at[pl.ds(0, batch), :], sem_o.at[0])]
    outs[0].start()
    fwds = [sib_own]

    def arrive(bits):
        sends[bits - 1].wait_recv()
        rows = pl.ds(bits * batch, batch)
        fwd = pltpu.make_async_remote_copy(src_ref=xs.at[rows, :], dst_ref=sib.at[rows, :], send_sem=sem_s.at[n_tp + bits - 1], recv_sem=sem_r.at[n_tp + bits - 1], device_id=peer(0, 1), device_id_type=MESH)
        fwd.start()
        fwds.append(fwd)
        out = pltpu.make_async_copy(xs.at[rows, :], ua_hbm.at[rows, :], sem_o.at[bits])
        out.start()
        outs.append(out)

    ffn_up(copies, True, xs, act, gate, up, 0, batch)
    arrive(1)
    arrive(2)
    ffn_up(copies, False, xs, act, gate, up, batch, 2 * batch)
    arrive(3)
    ffn_up(copies, False, xs, act, gate, up, 3 * batch, batch)
    for cp in copies[2]:
        cp.wait()
    for col in range(0, hidden, N_STEP):
        res = dot_nn(act[...], down[:, col:col + N_STEP])
        for blk in range(n_tp):
            parts[blk][:, col:col + N_STEP] = res[blk * batch:(blk + 1) * batch, :].astype(BF)
    for bits, fwd in enumerate(fwds):
        fwd.wait_recv()
        out = pltpu.make_async_copy(sib.at[pl.ds(bits * batch, batch), :], ua_hbm.at[pl.ds((n_tp + bits) * batch, batch), :], sem_o.at[n_tp + bits])
        out.start()
        outs.append(out)
    for cp in metas:
        cp.wait_recv()
    for slot in range(1, 2 * n_tp):
        ma_ref[slot] = msib[slot]
    for cp in sends + fwds + metas:
        cp.wait_send()
    for cp in outs:
        cp.wait()


def ffn0_call(u, meta, gate_t, up_t, down, n_tp):
    batch, hidden = u.shape
    ff = down.shape[0]
    n_f = -(-ff // F_STEP)
    n_dev = 2 * n_tp
    vm = pl.BlockSpec(memory_space=pltpu.VMEM)
    hb = pl.BlockSpec(memory_space=pl.ANY)
    return pl.pallas_call(
        ffn0_kernel,
        out_shape=[jax.ShapeDtypeStruct((batch, hidden), BF)] * n_tp + [jax.ShapeDtypeStruct((n_dev * batch, hidden), BF), jax.ShapeDtypeStruct((n_dev,) + meta.shape, F32)],
        in_specs=[vm, vm, hb, hb, hb],
        out_specs=[vm] * n_tp + [hb, vm],
        scratch_shapes=[
            pltpu.VMEM((ff, hidden), BF),
            pltpu.VMEM((ff, hidden), BF),
            pltpu.VMEM((ff, hidden), BF),
            pltpu.VMEM((n_tp * batch, hidden), BF),
            pltpu.VMEM((n_tp * batch, hidden), BF),
            pltpu.VMEM((n_tp * batch, ff), BF),
            pltpu.VMEM((n_dev,) + meta.shape, F32),
            pltpu.SemaphoreType.DMA((3, n_f)),
            pltpu.SemaphoreType.DMA((2 * n_tp - 1,)),
            pltpu.SemaphoreType.DMA((2 * n_tp - 1,)),
            pltpu.SemaphoreType.DMA((2, n_dev)),
            pltpu.SemaphoreType.DMA((n_dev,)),
        ],
        compiler_params=pltpu.CompilerParams(vmem_limit_bytes=VMEM_BYTES, collective_id=0, has_side_effects=True),
        cost_estimate=pl.CostEstimate(flops=6 * n_tp * batch * hidden * ff, bytes_accessed=6 * hidden * ff, transcendentals=n_tp * batch * ff),
        name="ffn0",
    )(u, meta, gate_t, up_t, down)


def ffn1_kernel(n_add, *refs):
    x_hbm = refs[:4]
    adds_hbm = refs[4:4 + n_add]
    h_ref, gate_hbm, up_hbm, down_hbm, y_ref, gate, up, down, xs, act, adds, own, sbuf, rbuf, sem_w, sem_x, sem_a, sem_s, sem_r = refs[4 + n_add:]
    n_tp = len(x_hbm)
    batch, hidden = h_ref.shape
    ff = gate.shape[0]
    i_tp = lax.axis_index('tp')
    i_ep = lax.axis_index('ep')
    order = (3, 1, 2, 0)
    x_cps = [pltpu.make_async_copy(x_hbm[blk], xs.at[pl.ds(pos * batch, batch), :], sem_x.at[pos]) for pos, blk in enumerate(order)]
    for cp in x_cps:
        cp.start()
    copies = weight_copies(((gate_hbm, gate), (up_hbm, up), (down_hbm, down)), sem_w, ff)
    for idx in range(len(copies[0])):
        copies[0][idx].start()
        copies[1][idx].start()
    n_own = n_add // 2
    own_cps = [pltpu.make_async_copy(adds_hbm[idx], adds.at[idx], sem_a.at[0, idx]) for idx in range(n_own)]
    for cp in copies[2]:
        cp.start()
    for cp in own_cps:
        cp.start()
    peers = [(jnp.bitwise_xor(i_tp, bits), i_ep) for bits in range(n_tp)]
    partner = (i_tp, 1 - i_ep)
    peer_barrier(peers[1:] + [partner])
    sib_cps = [pltpu.make_async_remote_copy(src_ref=adds_hbm[idx], dst_ref=adds.at[idx], send_sem=sem_a.at[1, idx], recv_sem=sem_a.at[0, idx], device_id=partner, device_id_type=MESH) for idx in range(n_own, n_add)]
    for cp in sib_cps:
        cp.start()
    sends = [None] + [pltpu.make_async_remote_copy(src_ref=sbuf.at[bits - 1], dst_ref=rbuf.at[bits - 1], send_sem=sem_s.at[bits - 1], recv_sem=sem_r.at[bits - 1], device_id=peers[bits], device_id_type=MESH) for bits in range(1, n_tp)]
    for cp in x_cps:
        cp.wait()
    for half in range(2):
        tok = 2 * half * batch
        ffn_up(copies, half == 0, xs, act, gate, up, tok, 2 * batch)
        if half == 0:
            for cp in copies[2]:
                cp.wait()
            for cp in own_cps:
                cp.wait()
            for cp in sib_cps:
                cp.wait_recv()
        for col in range(0, hidden, N_STEP):
            res = dot_nn(act[tok:tok + 2 * batch, :], down[:, col:col + N_STEP])
            for sub in range(2):
                blk = order[2 * half + sub]
                val = res[sub * batch:(sub + 1) * batch, :]
                for idx in range(n_add):
                    val = val + adds[idx, blk * batch:(blk + 1) * batch, col:col + N_STEP].astype(F32)
                if blk:
                    sbuf[blk - 1, :, col:col + N_STEP] = val.astype(BF)
                else:
                    own[:, col:col + N_STEP] = val + h_ref[:, col:col + N_STEP].astype(F32)
        for sub in range(2):
            blk = order[2 * half + sub]
            if blk:
                sends[blk].start()
    for cp in sends[1:]:
        cp.wait_recv()
    y_ref[...] = (own[...] + rbuf[0].astype(F32) + rbuf[1].astype(F32) + rbuf[2].astype(F32)).astype(BF)
    for cp in sends[1:] + sib_cps:
        cp.wait_send()


def ffn1_call(x_blocks, adds, h, gate_t, up_t, down):
    n_tp = len(x_blocks)
    batch, hidden = h.shape
    ff = down.shape[0]
    n_f = -(-ff // F_STEP)
    vm = pl.BlockSpec(memory_space=pltpu.VMEM)
    hb = pl.BlockSpec(memory_space=pl.ANY)
    return pl.pallas_call(
        functools.partial(ffn1_kernel, len(adds)),
        out_shape=jax.ShapeDtypeStruct((batch, hidden), BF),
        in_specs=[hb] * (n_tp + len(adds)) + [vm] + [hb] * 3,
        out_specs=vm,
        scratch_shapes=[
            pltpu.VMEM((ff, hidden), BF),
            pltpu.VMEM((ff, hidden), BF),
            pltpu.VMEM((ff, hidden), BF),
            pltpu.VMEM((n_tp * batch, hidden), BF),
            pltpu.VMEM((n_tp * batch, ff), BF),
            pltpu.VMEM((len(adds), n_tp * batch, hidden), BF),
            pltpu.VMEM((batch, hidden), F32),
            pltpu.VMEM((n_tp - 1, batch, hidden), BF),
            pltpu.VMEM((n_tp - 1, batch, hidden), BF),
            pltpu.SemaphoreType.DMA((3, n_f)),
            pltpu.SemaphoreType.DMA((n_tp,)),
            pltpu.SemaphoreType.DMA((2, len(adds))),
            pltpu.SemaphoreType.DMA((n_tp - 1,)),
            pltpu.SemaphoreType.DMA((n_tp - 1,)),
        ],
        compiler_params=pltpu.CompilerParams(vmem_limit_bytes=VMEM_BYTES, collective_id=1, has_side_effects=True),
        cost_estimate=pl.CostEstimate(flops=6 * n_tp * batch * hidden * ff, bytes_accessed=6 * hidden * ff, transcendentals=n_tp * batch * ff),
        name="ffn1",
    )(*x_blocks, *adds, h, gate_t, up_t, down)


ROW_TILE = 128


def moe_kernel(exp_local, ids_ref, wts_ref, base_ref, xs, gate_ref, up_ref, down_ref, own_ref, sib_ref, acc, rank_s, wrow_s, cnt_s):
    exp = pl.program_id(0)
    top_k, n_tok = ids_ref.shape
    hidden = xs.shape[1]

    @pl.when(exp == 0)
    def _():
        acc[...] = jnp.zeros_like(acc)
        local = ids_ref[...] - base_ref[0]
        lane = lax.broadcasted_iota(jnp.int32, (1, n_tok), 1)
        for idx in range(exp_local):
            eq = local == idx
            hit = jnp.max(jnp.where(eq, 1.0, 0.0), axis=0, keepdims=True)
            wrow_s[idx] = jnp.sum(jnp.where(eq, wts_ref[...], 0.0), axis=0, keepdims=True)
            run = hit
            shift = 1
            while shift < n_tok:
                run = run + jnp.where(lane >= shift, pltpu.roll(run, shift, 1), 0.0)
                shift *= 2
            rank_s[idx] = jnp.where(hit > 0.5, run - 1.0, -1.0).astype(jnp.int32)
            cnt_s[idx] = jnp.sum(hit).astype(jnp.int32)

    count = cnt_s[exp]
    rank = rank_s[exp]
    wrow = wrow_s[exp]

    def tile(step, carry):
        row_i = lax.broadcasted_iota(jnp.int32, (ROW_TILE, n_tok), 0) + step * ROW_TILE
        pick = row_i == rank
        pick_b = jnp.where(pick, 1.0, 0.0).astype(BF)
        w_col = jnp.sum(jnp.where(pick, wrow, 0.0), axis=1, keepdims=True)
        x_t = dot_nn(pick_b, xs[...]).astype(BF)
        g_val = dot_nn(x_t, gate_ref[0])
        u_val = dot_nn(x_t, up_ref[0])
        act = silu_mul(g_val, u_val)
        n_step = 512
        for col in range(0, hidden, n_step):
            y_val = (dot_nn(act, down_ref[0, :, col:col + n_step]) * w_col).astype(BF)
            acc[:, col:col + n_step] += dot_tn(pick_b, y_val)
        return carry

    lax.fori_loop(0, (count + ROW_TILE - 1) // ROW_TILE, tile, 0)

    @pl.when(exp == exp_local - 1)
    def _():
        half = n_tok // 2
        own_ref[...] = acc[0:half, :].astype(BF)
        sib_ref[...] = acc[half:n_tok, :].astype(BF)


def moe_call(ids, wts, base, x_all, exp_gate, exp_up, exp_down, first, n_exp):
    _, hidden, ff = exp_gate.shape
    n_tok = ids.shape[1]
    one = pl.Buffered(1)

    def whole(shape):
        return pl.BlockSpec(shape, lambda e: (0,) * len(shape), pipeline_mode=one)

    return pl.pallas_call(
        functools.partial(moe_kernel, n_exp),
        out_shape=[jax.ShapeDtypeStruct((n_tok // 2, hidden), BF)] * 2,
        grid=(n_exp,),
        in_specs=[whole(ids.shape), whole(wts.shape), pl.BlockSpec(memory_space=pltpu.SMEM), whole(x_all.shape)]
        + [pl.BlockSpec((1, hidden, ff), lambda e: (e + first, 0, 0)), pl.BlockSpec((1, hidden, ff), lambda e: (e + first, 0, 0)), pl.BlockSpec((1, ff, hidden), lambda e: (e + first, 0, 0))],
        out_specs=[whole((n_tok // 2, hidden))] * 2,
        scratch_shapes=[
            pltpu.VMEM((n_tok, hidden), F32),
            pltpu.VMEM((n_exp, 1, n_tok), jnp.int32),
            pltpu.VMEM((n_exp, 1, n_tok), F32),
            pltpu.SMEM((n_exp,), jnp.int32),
        ],
        compiler_params=pltpu.CompilerParams(dimension_semantics=("arbitrary",), vmem_limit_bytes=VMEM_BYTES),
        cost_estimate=pl.CostEstimate(flops=10 ** 10, bytes_accessed=6 * n_exp * hidden * ff, transcendentals=10 ** 6),
        name="moe",
    )(ids, wts, base + first, x_all, exp_gate, exp_up, exp_down)


def solution(mesh):
    n_tp = mesh.shape['tp']
    tok_spec = P(('tp', 'ep'))
    rep_spec = P()
    col_spec = P(None, 'tp')
    row_spec = P('tp', None)
    in_specs = (tok_spec, tok_spec, tok_spec, tok_spec, tok_spec, tok_spec, rep_spec, rep_spec, rep_spec, rep_spec, rep_spec, rep_spec, rep_spec, rep_spec, col_spec, col_spec, row_spec, col_spec, col_spec, row_spec, tok_spec, tok_spec, tok_spec)

    def swap_tp(val, bits):
        return lax.ppermute(val, 'tp', [(i, i ^ bits) for i in range(n_tp)])

    def gather_tp(val):
        return [val] + [swap_tp(val, bits) for bits in range(1, n_tp)]

    def layer_step(hidden_in, kv_cache0, kv_cache1, kv_lens, route_ids, route_wts, attn0_q, attn0_uk, attn0_uv, attn0_out, attn1_q, attn1_uk, attn1_uv, attn1_out, ffn0_gate, ffn0_up, ffn0_down, ffn1_gate, ffn1_up, ffn1_down, exp_gate, exp_up, exp_down):
        batch = hidden_in.shape[0]
        exp_local = exp_gate.shape[0]
        rope = kv_cache0.shape[2] - attn0_uk.shape[2]
        i_tp = lax.axis_index('tp')
        i_ep = lax.axis_index('ep')
        half = rope // 2
        inv_freq = ROPE_BASE ** (-2.0 * jnp.arange(half, dtype=F32) / rope)
        angle = kv_lens.astype(F32)[:, None] * jnp.tile(inv_freq, 128 // half)
        cos_t = jnp.cos(angle)
        sign = jnp.where(jnp.arange(128) % rope < half, -1.0, 1.0).astype(F32)
        sin_t = jnp.sin(angle) * sign
        lens_b = jnp.broadcast_to(kv_lens[:, None], (batch, 128))

        top_k = route_ids.shape[1]
        pad = jnp.zeros((16 - 2 * top_k, batch), F32)
        meta = jnp.concatenate([route_ids.T.astype(F32), route_wts.T, pad], axis=0)
        base = ((i_tp * 2 + i_ep) * exp_local).astype(jnp.int32).reshape(1)

        def t_kv(cache):
            return jnp.transpose(cache, (1, 2, 0))

        h0, u0 = mla_call(hidden_in, [], lens_b, cos_t, sin_t, t_kv(kv_cache0), jnp.transpose(attn0_q, (1, 2, 0)), attn0_uk, attn0_uv, attn0_out)
        outs = ffn0_call(u0, meta, ffn0_gate.T, ffn0_up.T, ffn0_down, n_tp)
        parts0, u_all, meta_all = outs[:n_tp], outs[n_tp], outs[n_tp + 1]
        recv0 = [parts0[0]] + [swap_tp(parts0[bits], bits) for bits in range(1, n_tp)]
        meta_t = jnp.transpose(meta_all, (1, 0, 2)).reshape(16, 2 * n_tp * batch)
        ids_all = meta_t[:top_k].astype(jnp.int32)
        wts_all = meta_t[top_k:2 * top_k]
        n_half = exp_local // 2
        ma_own, ma_sib = moe_call(ids_all, wts_all, base, u_all, exp_gate, exp_up, exp_down, 0, n_half)
        h1, v0 = mla_call(h0, recv0, lens_b, cos_t, sin_t, t_kv(kv_cache1), jnp.transpose(attn1_q, (1, 2, 0)), attn1_uk, attn1_uv, attn1_out)
        v_own = gather_tp(v0)
        u_late, ids_late, h1 = lax.optimization_barrier((u_all, ids_all, h1))
        mb_own, mb_sib = moe_call(ids_late, wts_all, base, u_late, exp_gate, exp_up, exp_down, n_half, exp_local - n_half)
        return ffn1_call(v_own, [ma_own, mb_own, ma_sib, mb_sib], h1, ffn1_gate.T, ffn1_up.T, ffn1_down)

    return jax.shard_map(layer_step, mesh=mesh, in_specs=in_specs, out_specs=tok_spec, check_vma=False)
```
